256 devices in a mesh: rep: 4 (over y), row: 16 (over z, core), col: 4 (over x).
Axes of the slice: x: 4, y: 4, z: 8, core: 2. Of those that a mesh axis runs over, the one named last changes fastest.
Arguments:
- acts: bfloat16 [4, 256, 5120], P('rep', None, 'row'), may hold values from -6 to 6
- grad_out: bfloat16 [4, 256, 13824], P('rep', None, 'col'), may hold values from -0.375 to 0.375
- momentum: bfloat16 [4, 5120, 13824], P('rep', 'row', 'col'), may hold values from -6 to 6
- q_basis: bfloat16 [640, 13824], P(None, 'col'), may hold values from -6 to 6
Outputs:
- momentum_next: bfloat16 [4, 5120, 13824], P('rep', 'row', 'col')
- q_next: bfloat16 [640, 13824], P('row', 'col')
- update: bfloat16 [5120, 13824], P('row', 'col')
The draws below stay inside these ranges and needn't reach their ends.
All inputs are finite; a program needn't handle non-finite values.
Results may differ from the reference program's by a relative error of at most 0.019.
Values may be sent and summed in bfloat16 or wider, within the bound.
No kernel may reach another device: no remote copies, remote signals or barrier semaphores. Data moves between devices by JAX's collectives and lax.ppermute only.
A program may use at most 128 MiB of HBM per device.

```python
import jax
import jax.numpy as jnp
from jax import lax

D = 5120
FF = 13824
RANK = 640
TOK = 256
REPS = 4


def block_scale(rng, dims, pieces, low, high):
    def one(axis_at, blocks):
        draws = jax.random.uniform(jax.random.fold_in(jax.random.fold_in(rng, 6), axis_at), (blocks,), jnp.float32, low / len(pieces), high / len(pieces))
        return jnp.repeat(jnp.exp(draws), dims[axis_at] // blocks).reshape((-1,) + (1,) * (len(dims) - axis_at - 1))

    level = one(*pieces[0])
    for cut in pieces[1:]:
        level = level * one(*cut)
    return level


def centred(key, dims, spread, limit, shards=(), kind=jnp.bfloat16):
    drawn = spread * jax.random.normal(key, dims, jnp.float32)
    if shards:
        drawn = drawn * block_scale(key, dims, shards, -0.22, 0.18)
    return jnp.clip(drawn, -limit, limit).astype(kind)


def setup_inputs(seed: int = 0) -> dict:
    key_of = jax.random.split(jax.random.key(seed), 5)
    return {
        "acts": centred(key_of[0], (REPS, TOK, D), 1.0, 6.0, ((0, 4), (2, 16))),
        "grad_out": centred(key_of[1], (REPS, TOK, FF), TOK ** -0.5, 0.375, ((0, 4), (2, 4))),
        "momentum": centred(key_of[2], (REPS, D, FF), 1.0, 6.0, ((0, 4), (1, 16), (2, 4))),
        "q_basis": centred(key_of[3], (RANK, FF), 1.0, 6.0, ((1, 4),)),
    }


keep_factor = 0.6

def reference(acts, grad_out, momentum, q_basis):
    left = jnp.zeros((D, RANK), jnp.float32)
    boosted_all = []
    for replica in range(REPS):
        grad = jnp.dot(acts[replica].T.astype(jnp.float32), grad_out[replica].astype(jnp.float32), preferred_element_type=jnp.float32)
        boosted = (momentum[replica].astype(jnp.float32) + grad).astype(jnp.bfloat16)
        boosted_all.append(boosted)
        left = left + jnp.dot(boosted.astype(jnp.float32), q_basis.T.astype(jnp.float32), preferred_element_type=jnp.float32)
    gram = jnp.dot(left.T, left, precision=lax.Precision.HIGHEST)
    chol = jnp.linalg.cholesky(gram)
    ortho = lax.linalg.triangular_solve(chol, left, left_side=False, lower=True, transpose_a=True).astype(jnp.bfloat16)
    right_sum = jnp.zeros((RANK, FF), jnp.float32)
    for replica in range(REPS):
        right_sum = right_sum + jnp.dot(ortho.T.astype(jnp.float32), boosted_all[replica].astype(jnp.float32), preferred_element_type=jnp.float32)
    right = (right_sum * (1.0 / REPS)).astype(jnp.bfloat16)
    right_wide = right.astype(jnp.float32)
    msq = lax.optimization_barrier(jnp.mean(right_wide * right_wide, axis=1))
    q_full = (right_wide * lax.rsqrt(msq + 1e-06)[:, None]).astype(jnp.bfloat16)
    feedback = jnp.dot(ortho.astype(jnp.float32), right.astype(jnp.float32), preferred_element_type=jnp.float32)
    momentum_next = jnp.stack([(boosted_all[replica].astype(jnp.float32) - (1.0 - keep_factor) * feedback).astype(jnp.bfloat16) for replica in range(REPS)])
    update = (jnp.sqrt(jnp.float32(D) / RANK) * jnp.dot(ortho.astype(jnp.float32), q_full.astype(jnp.float32), preferred_element_type=jnp.float32)).astype(jnp.bfloat16)
    return (momentum_next, q_full, update)
```

```python
import functools

import jax
import jax.numpy as jnp
from jax import lax
from jax.experimental import pallas as pl
from jax.experimental.pallas import tpu as pltpu
from jax.sharding import Mesh
from jax.sharding import PartitionSpec as P

RANK = 640
ROW = ("row_0", "row_1")
PLANE = ("rep", "col")
BLOCK = 128
SUB = 32

keep_factor = 0.6


def dot(a, b, dims, exact=False):
    return lax.dot_general(
        a,
        b,
        (dims, ((), ())),
        precision=lax.Precision.HIGHEST if exact else None,
        preferred_element_type=jnp.float32,
    )


def eliminated(tile, panel, first):
    groups = SUB // 8
    row = lax.broadcasted_iota(jnp.int32, (8, BLOCK), 0)

    def spread(x, at):
        return jnp.broadcast_to(x[at : at + 1, :], (8, BLOCK))

    column = [[None] * groups for _ in range(SUB)]
    factor = [[None] * groups for _ in range(SUB)]
    kept = [panel[8 * g : 8 * g + 8, :] for g in range(groups)]
    pivots = [None] * groups
    for k in range(SUB):
        own, at = divmod(k, 8)
        for g in range(own, groups):
            lone = tile[8 * g : 8 * g + 8, first + k : first + k + 1]
            column[k][g] = jnp.broadcast_to(lone, (8, BLOCK))
        for j in range(k):
            across = spread(column[j][own], at)
            for g in range(own, groups):
                column[k][g] = column[k][g] - factor[j][g] * across
        pivot = spread(column[k][own], at)
        pivots[own] = pivot if at == 0 else jnp.where(row == at, pivot, pivots[own])
        inverse = 1.0 / pivot
        source = spread(kept[own], at)
        for g in range(own, groups):
            scaled = column[k][g] * inverse
            if g == own:
                scaled = jnp.where(row > at, scaled, 0.0)
            factor[k][g] = scaled
            kept[g] = kept[g] - scaled * source
    out = []
    for g in range(groups):
        y = lax.rsqrt(pivots[g])
        y = y * (1.5 - 0.5 * pivots[g] * y * y)
        out.append(kept[g] * y)
    return jnp.concatenate(out, axis=0)


def factor_kernel(blocks, gram_ref, out_ref, tile_ref):
    out_ref[...] = gram_ref[...]
    lane = lax.broadcasted_iota(jnp.int32, (SUB, BLOCK), 1)
    line = lax.broadcasted_iota(jnp.int32, (SUB, BLOCK), 0)
    below = lax.broadcasted_iota(jnp.int32, (BLOCK, BLOCK), 0)
    right = lax.broadcasted_iota(jnp.int32, (BLOCK, BLOCK), 1)

    @pl.loop(0, blocks)
    def _(k):
        here = pl.ds(pl.multiple_of(k * BLOCK, BLOCK), BLOCK)
        tile_ref[...] = out_ref[here, here]
        for s in range(BLOCK // SUB):
            low, high = s * SUB, (s + 1) * SUB
            tile = tile_ref[low:high, :]
            unit = (lane - low == line).astype(jnp.float32)
            panel = jnp.where((lane >= low) & (lane < high), unit, tile)
            done = eliminated(tile, panel, low)
            tile_ref[low:high, :] = done
            if high < BLOCK:
                gone = right[high:, :] // SUB == s
                rest = jnp.where(gone, 0.0, tile_ref[high:, :])
                tile_ref[high:, :] = rest - dot(done.T[high:, :], done, ((1,), (0,)), True)
        own = jnp.where(right <= below, tile_ref[...], 0.0)
        out_ref[here, :] = dot(own, out_ref[here, :], ((1,), (0,)), True)
        out_ref[here, here] = own

        @pl.loop(k + 1, blocks)
        def _(i):
            there = pl.ds(pl.multiple_of(i * BLOCK, BLOCK), BLOCK)
            panel = out_ref[here, there].T
            out_ref[there, here] = jnp.zeros((BLOCK, BLOCK), jnp.float32)
            out_ref[there, :] = out_ref[there, :] - dot(panel, out_ref[here, :], ((1,), (0,)), True)

    for k in range(blocks):
        here = slice(k * BLOCK, (k + 1) * BLOCK)
        whole = out_ref[here, :]
        lower = lax.broadcasted_iota(jnp.int32, whole.shape, 1) <= (
            lax.broadcasted_iota(jnp.int32, whole.shape, 0) + k * BLOCK
        )
        out_ref[here, :] = jnp.where(lower, whole, 0.0)


def inverse_factor(gram):
    size = gram.shape[0]
    return pl.pallas_call(
        functools.partial(factor_kernel, size // BLOCK),
        out_shape=jax.ShapeDtypeStruct((size, size), jnp.float32),
        in_specs=[pl.BlockSpec(memory_space=pltpu.VMEM)],
        out_specs=pl.BlockSpec(memory_space=pltpu.VMEM),
        scratch_shapes=[pltpu.VMEM((BLOCK, BLOCK), jnp.float32)],
        cost_estimate=pl.CostEstimate(
            flops=20_000_000_000, bytes_accessed=8 * size * size, transcendentals=0
        ),
        name="inverse_factor",
    )(gram)


def summed_at_owner(x, axes):
    return jnp.sum(lax.all_to_all(x, axes, 0, 0, tiled=True), axis=0)


def from_all(x, axes):
    peers = lax.axis_size(axes)
    return lax.all_to_all(jnp.broadcast_to(x[None], (peers, *x.shape)), axes, 0, 0, tiled=True)


def from_other_core(x):
    return lax.ppermute(x, "row_1", [(0, 1), (1, 0)])


def sum_over(x, axis):
    peers = lax.axis_size(axis)
    terms = [x] + [
        lax.ppermute(x, axis, [(i, (i + step) % peers) for i in range(peers)])
        for step in range(1, peers)
    ]
    return sum(terms[1:], terms[0])


def both_cores(mine, theirs, first, axis):
    return jnp.stack([jnp.where(first, mine, theirs), jnp.where(first, theirs, mine)], axis)


def shards(acts, grad_out, momentum, q_basis):
    first = lax.axis_index("row_1") == 0
    grad = dot(acts[0], grad_out[0], ((0,), (0,)))
    boosted = (momentum[0].astype(jnp.float32) + grad).astype(jnp.bfloat16)
    height, width = boosted.shape
    replicas, columns = lax.axis_size("rep"), lax.axis_size("col")
    chips = lax.axis_size("row_0")
    plane = replicas * columns
    lines = RANK // plane
    strip = width // replicas
    short = strip // (2 * chips)

    same = jnp.eye(height, dtype=jnp.bfloat16)
    turned = dot(boosted, same, ((0,), (0,))).reshape(replicas, strip, height)
    total = lax.psum_scatter(turned, "rep", scatter_dimension=0, tiled=False)

    partial_left = dot(q_basis, boosted, ((1,), (1,)))
    mine = summed_at_owner(partial_left.reshape(plane, lines, height), PLANE)
    left = from_all(mine, PLANE).reshape(RANK, height)

    halves = dot(mine, left, ((1,), (1,)), True).reshape(2, lines // 2, RANK)
    kept = jnp.where(first, halves[0], halves[1])
    given = jnp.where(first, halves[1], halves[0])
    half = jnp.sum(from_all(kept + from_other_core(given), "row_0"), axis=0)
    known = from_all(half, PLANE)
    gram = both_cores(known, from_other_core(known), first, 1).reshape(RANK, RANK)

    product = dot(total, left, ((1,), (1,)), True)
    product = product.reshape(2, chips, short, RANK).swapaxes(0, 1)
    share = lax.psum_scatter(
        product.reshape(2 * chips, short, RANK), ROW, scatter_dimension=0, tiled=False
    )

    inverse = inverse_factor(gram)
    ortho = dot(left, inverse, ((0,), (1,)), True).astype(jnp.bfloat16)
    piece = (dot(share, inverse, ((1,), (1,)), True) * (1.0 / replicas)).astype(jnp.bfloat16)
    chips_pieces = from_all(piece, "row_0").reshape(chips * short, RANK)
    known_right = from_all(chips_pieces, "rep")
    right = both_cores(known_right, from_other_core(known_right), first, 1).reshape(width, RANK)

    wide = right.astype(jnp.float32)
    squares = sum_over(jnp.sum(wide * wide, axis=0), "col")
    scale = lax.rsqrt(squares / (width * columns) + 1e-06)
    feedback = dot(ortho, right, ((1,), (1,)))
    momentum_next = (boosted.astype(jnp.float32) - (1.0 - keep_factor) * feedback).astype(
        jnp.bfloat16
    )[None]
    q_full = (wide * scale[None, :]).astype(jnp.bfloat16)
    block = RANK // lax.axis_size(ROW)
    wanted = lax.axis_index(ROW) * block + lax.broadcasted_iota(jnp.int32, (block, RANK), 0)
    chosen = (lax.broadcasted_iota(jnp.int32, (block, RANK), 1) == wanted).astype(jnp.bfloat16)
    q_next = dot(chosen, q_full, ((1,), (1,))).astype(jnp.bfloat16)
    height_all = height * lax.axis_size(ROW)
    update = (
        jnp.sqrt(jnp.float32(height_all) / RANK) * dot(ortho, q_full, ((1,), (1,)))
    ).astype(jnp.bfloat16)
    return (momentum_next, q_next, update)


def solution(mesh):
    split = Mesh(
        mesh.devices.reshape(mesh.shape["rep"], 8, 2, mesh.shape["col"]),
        ("rep", "row_0", "row_1", "col"),
    )
    return jax.shard_map(
        shards,
        mesh=split,
        in_specs=(P("rep", None, ROW), P("rep", None, "col"), P("rep", ROW, "col"), P(None, "col")),
        out_specs=(P("rep", ROW, "col"), P(ROW, "col"), P(ROW, "col")),
        check_vma=False,
    )
```

```python
import functools

import jax
import jax.numpy as jnp
from jax import lax
from jax.experimental import pallas as pl
from jax.experimental.pallas import tpu as pltpu
from jax.sharding import Mesh
from jax.sharding import PartitionSpec as P


ROW = ("row_0", "row_1")
PLANE = ("rep", "col")
BLOCK = 128
SUB = 32

keep_factor = 0.6


def dot(a, b, dims, exact=False):
    return lax.dot_general(
        a,
        b,
        (dims, ((), ())),
        precision=lax.Precision.HIGHEST if exact else None,
        preferred_element_type=jnp.float32,
    )


def eliminated(tile, panel, first):
    groups = SUB // 8
    row = lax.broadcasted_iota(jnp.int32, (8, BLOCK), 0)

    def spread(x, at):
        return jnp.broadcast_to(x[at : at + 1, :], (8, BLOCK))

    column = [[None] * groups for _ in range(SUB)]
    factor = [[None] * groups for _ in range(SUB)]
    kept = [panel[8 * g : 8 * g + 8, :] for g in range(groups)]
    pivots = [None] * groups
    for k in range(SUB):
        own, at = divmod(k, 8)
        for g in range(own, groups):
            lone = tile[8 * g : 8 * g + 8, first + k : first + k + 1]
            column[k][g] = jnp.broadcast_to(lone, (8, BLOCK))
        for j in range(k):
            across = spread(column[j][own], at)
            for g in range(own, groups):
                column[k][g] = column[k][g] - factor[j][g] * across
        pivot = spread(column[k][own], at)
        pivots[own] = pivot if at == 0 else jnp.where(row == at, pivot, pivots[own])
        inverse = 1.0 / pivot
        source = spread(kept[own], at)
        for g in range(own, groups):
            scaled = column[k][g] * inverse
            if g == own:
                scaled = jnp.where(row > at, scaled, 0.0)
            factor[k][g] = scaled
            kept[g] = kept[g] - scaled * source
    out = []
    for g in range(groups):
        y = lax.rsqrt(pivots[g])
        y = y * (1.5 - 0.5 * pivots[g] * y * y)
        out.append(kept[g] * y)
    return jnp.concatenate(out, axis=0)


def factor_kernel(blocks, core_ref, mine_ref, theirs_ref, out_ref, tile_ref):
    groups, lines, _ = mine_ref.shape
    first = core_ref[0] == 0
    for p in range(groups):
        mine, theirs = mine_ref[p], theirs_ref[p]
        start = 2 * p * lines
        out_ref[start : start + lines, :] = jnp.where(first, mine, theirs)
        out_ref[start + lines : start + 2 * lines, :] = jnp.where(first, theirs, mine)
    lane = lax.broadcasted_iota(jnp.int32, (SUB, BLOCK), 1)
    line = lax.broadcasted_iota(jnp.int32, (SUB, BLOCK), 0)
    below = lax.broadcasted_iota(jnp.int32, (BLOCK, BLOCK), 0)
    right = lax.broadcasted_iota(jnp.int32, (BLOCK, BLOCK), 1)

    @pl.loop(0, blocks)
    def _(k):
        here = pl.ds(pl.multiple_of(k * BLOCK, BLOCK), BLOCK)
        tile_ref[...] = out_ref[here, here]
        for s in range(BLOCK // SUB):
            low, high = s * SUB, (s + 1) * SUB
            tile = tile_ref[low:high, :]
            unit = (lane - low == line).astype(jnp.float32)
            panel = jnp.where((lane >= low) & (lane < high), unit, tile)
            done = eliminated(tile, panel, low)
            tile_ref[low:high, :] = done
            if high < BLOCK:
                gone = right[high:, :] // SUB == s
                rest = jnp.where(gone, 0.0, tile_ref[high:, :])
                tile_ref[high:, :] = rest - dot(done.T[high:, :], done, ((1,), (0,)), True)
        own = jnp.where(right <= below, tile_ref[...], 0.0)
        out_ref[here, :] = dot(own, out_ref[here, :], ((1,), (0,)), True)
        out_ref[here, here] = own

        @pl.loop(k + 1, blocks)
        def _(i):
            there = pl.ds(pl.multiple_of(i * BLOCK, BLOCK), BLOCK)
            panel = out_ref[here, there].T
            out_ref[there, here] = jnp.zeros((BLOCK, BLOCK), jnp.float32)
            out_ref[there, :] = out_ref[there, :] - dot(panel, out_ref[here, :], ((1,), (0,)), True)

    for k in range(blocks):
        here = slice(k * BLOCK, (k + 1) * BLOCK)
        whole = out_ref[here, :]
        lower = lax.broadcasted_iota(jnp.int32, whole.shape, 1) <= (
            lax.broadcasted_iota(jnp.int32, whole.shape, 0) + k * BLOCK
        )
        out_ref[here, :] = jnp.where(lower, whole, 0.0)


def inverse_factor(core, mine, theirs):
    size = mine.shape[-1]
    return pl.pallas_call(
        functools.partial(factor_kernel, size // BLOCK),
        out_shape=jax.ShapeDtypeStruct((size, size), jnp.float32),
        in_specs=[pl.BlockSpec(memory_space=pltpu.SMEM)]
        + [pl.BlockSpec(memory_space=pltpu.VMEM)] * 2,
        out_specs=pl.BlockSpec(memory_space=pltpu.VMEM),
        scratch_shapes=[pltpu.VMEM((BLOCK, BLOCK), jnp.float32)],
        cost_estimate=pl.CostEstimate(
            flops=20_000_000_000, bytes_accessed=8 * size * size, transcendentals=0
        ),
        name="inverse_factor",
    )(core, mine, theirs)


def summed_at_owner(x, axes):
    return jnp.sum(lax.all_to_all(x, axes, 0, 0, tiled=True), axis=0)


def from_all(x, axes):
    peers = lax.axis_size(axes)
    return lax.all_to_all(jnp.broadcast_to(x[None], (peers, *x.shape)), axes, 0, 0, tiled=True)


def from_other_core(x):
    return lax.ppermute(x, "row_1", [(0, 1), (1, 0)])


def shifted(x, axis, step):
    peers = lax.axis_size(axis)
    return lax.ppermute(x, axis, [(i, (i + step) % peers) for i in range(peers)])


def sum_over(x, axis):
    terms = [shifted(x, axis, step) for step in range(1, lax.axis_size(axis))]
    return sum(terms, x)


def around(index, axis):
    return index & (lax.axis_size(axis) - 1)


def terms_at_owner(x, axis, dim):
    peers, me = lax.axis_size(axis), lax.axis_index(axis)
    lines = x.shape[dim] // peers

    def part(step):
        return lax.dynamic_slice_in_dim(x, around(me + step, axis) * lines, lines, dim)

    return [part(0)] + [shifted(part(step), axis, step) for step in range(1, peers)]


def gathered_directly(piece, axis):
    peers, me = lax.axis_size(axis), lax.axis_index(axis)
    whole = jnp.zeros((peers, *piece.shape), piece.dtype)
    for step in range(peers):
        term = shifted(piece, axis, step) if step else piece
        whole = lax.dynamic_update_slice(whole, term[None], (around(me - step, axis), 0, 0))
    return whole.reshape(-1, piece.shape[-1])


def gathered_by_ring(block, core):
    peers, me = lax.axis_size("rep"), lax.axis_index("rep")
    lines, rank = block.shape
    cut = lines // 2
    whole = jnp.zeros((peers, 2, lines, rank), block.dtype)

    def both(whole, part, step, line):
        replica = around(me + step, "rep")
        for side, term in ((core, part), (1 - core, from_other_core(part))):
            whole = lax.dynamic_update_slice(whole, term[None, None], (replica, side, line, 0))
        return whole

    upper, lower = block[:cut], block[cut:]
    up_upper, down_lower = shifted(upper, "rep", 1), shifted(lower, "rep", -1)
    up_lower, down_upper = shifted(lower, "rep", 1), shifted(upper, "rep", -1)
    far_upper, far_lower = shifted(up_upper, "rep", 1), shifted(down_lower, "rep", -1)
    whole = both(whole, block, 0, 0)
    whole = both(whole, up_upper, -1, 0)
    whole = both(whole, down_lower, 1, cut)
    whole = both(whole, up_lower, -1, cut)
    whole = both(whole, down_upper, 1, 0)
    whole = both(whole, far_upper, -2, 0)
    return both(whole, far_lower, 2, cut)


def shards(acts, grad_out, momentum, q_basis):
    core = lax.axis_index("row_1")
    grad = dot(acts[0], grad_out[0], ((0,), (0,)))
    boosted = (momentum[0].astype(jnp.float32) + grad).astype(jnp.bfloat16)
    height, width = boosted.shape
    rank = q_basis.shape[0]
    replicas, columns = lax.axis_size("rep"), lax.axis_size("col")
    plane = replicas * columns
    strip = width // (2 * replicas)

    terms = terms_at_owner(boosted, "rep", 1)

    partial_left = dot(boosted, q_basis, ((1,), (1,)))
    mine = summed_at_owner(partial_left.reshape(plane, height // plane, rank), PLANE)
    left = from_all(mine, PLANE).reshape(height, rank)

    gram = dot(left, left, ((0,), (0,)), True)
    lines = rank // (2 * plane)
    place = 2 * (lax.axis_index("rep") * columns + lax.axis_index("col"))
    kept = lax.dynamic_slice_in_dim(gram, (place + core) * lines, lines, 0)
    given = lax.dynamic_slice_in_dim(gram, (place + 1 - core) * lines, lines, 0)
    half = jnp.sum(from_all(kept + from_other_core(given), "row_0"), axis=0)
    known = from_all(half, PLANE)
    inverse = inverse_factor(core.reshape(1), known, from_other_core(known))

    total = sum(term.astype(jnp.float32) for term in terms)
    product = dot(total, left, ((0,), (0,)), True)
    ours = lax.dynamic_slice_in_dim(product, core * strip, strip, 0)
    other = lax.dynamic_slice_in_dim(product, (1 - core) * strip, strip, 0)
    share = sum(terms_at_owner(ours + from_other_core(other), "row_0", 0))

    ortho = dot(left, inverse, ((1,), (1,)), True).astype(jnp.bfloat16)
    piece = (dot(share, inverse, ((1,), (1,)), True) * (1.0 / replicas)).astype(jnp.bfloat16)
    right = gathered_by_ring(gathered_directly(piece, "row_0"), core).reshape(width, rank)

    wide = right.astype(jnp.float32)
    squares = sum_over(jnp.sum(wide * wide, axis=0), "col")
    scale = lax.rsqrt(squares / (width * columns) + 1e-06)
    feedback = dot(ortho, right, ((1,), (1,)))
    momentum_next = (boosted.astype(jnp.float32) - (1.0 - keep_factor) * feedback).astype(
        jnp.bfloat16
    )[None]
    q_full = (wide * scale[None, :]).astype(jnp.bfloat16)
    rows = rank // lax.axis_size(ROW)
    wanted = lax.axis_index(ROW) * rows + lax.broadcasted_iota(jnp.int32, (rows, rank), 0)
    chosen = (lax.broadcasted_iota(jnp.int32, (rows, rank), 1) == wanted).astype(jnp.bfloat16)
    q_next = dot(chosen, q_full, ((1,), (1,))).astype(jnp.bfloat16)
    height_all = height * lax.axis_size(ROW)
    update = (
        jnp.sqrt(jnp.float32(height_all) / rank) * dot(ortho, q_full, ((1,), (1,)))
    ).astype(jnp.bfloat16)
    return (momentum_next, q_next, update)


def solution(mesh):
    split = Mesh(
        mesh.devices.reshape(mesh.shape["rep"], 8, 2, mesh.shape["col"]),
        ("rep", "row_0", "row_1", "col"),
    )

    return jax.shard_map(
        shards,
        mesh=split,
        in_specs=(P("rep", None, ROW), P("rep", None, "col"), P("rep", ROW, "col"), P(None, "col")),
        out_specs=(P("rep", ROW, "col"), P(ROW, "col"), P(ROW, "col")),
        check_vma=False,
    )
```

```python
import functools

import jax
import jax.numpy as jnp
from jax import lax
from jax.experimental import pallas as pl
from jax.experimental.pallas import tpu as pltpu
from jax.sharding import Mesh
from jax.sharding import PartitionSpec as P


ROW = ("row_0", "row_1")
PLANE = ("rep", "col")
BLOCK = 128
SUB = 32
EXACT = lax.Precision.HIGHEST
CLOSE = lax.Precision.HIGH

keep_factor = 0.6


def dot(a, b, dims, precision=None):
    return lax.dot_general(
        a,
        b,
        (dims, ((), ())),
        precision=precision,
        preferred_element_type=jnp.float32,
    )


def eliminated(tile, panel, first):
    groups = SUB // 8
    row = lax.broadcasted_iota(jnp.int32, (8, BLOCK), 0)

    def spread(x, at):
        return jnp.broadcast_to(x[at : at + 1, :], (8, BLOCK))

    column = [[None] * groups for _ in range(SUB)]
    factor = [[None] * groups for _ in range(SUB)]
    kept = [panel[8 * g : 8 * g + 8, :] for g in range(groups)]
    pivots = [None] * groups
    for k in range(SUB):
        own, at = divmod(k, 8)
        for g in range(own, groups):
            lone = tile[8 * g : 8 * g + 8, first + k : first + k + 1]
            column[k][g] = jnp.broadcast_to(lone, (8, BLOCK))
        for j in range(k):
            across = spread(column[j][own], at)
            for g in range(own, groups):
                column[k][g] = column[k][g] - factor[j][g] * across
        pivot = spread(column[k][own], at)
        pivots[own] = pivot if at == 0 else jnp.where(row == at, pivot, pivots[own])
        inverse = 1.0 / pivot
        source = spread(kept[own], at)
        for g in range(own, groups):
            scaled = column[k][g] * inverse
            if g == own:
                scaled = jnp.where(row > at, scaled, 0.0)
            factor[k][g] = scaled
            kept[g] = kept[g] - scaled * source
    out = []
    for g in range(groups):
        y = lax.rsqrt(pivots[g])
        y = y * (1.5 - 0.5 * pivots[g] * y * y)
        out.append(kept[g] * y)
    return jnp.concatenate(out, axis=0)


def factor_kernel(blocks, lines, core_ref, mine_ref, theirs_ref, out_ref, tile_ref):
    groups = mine_ref.shape[0]
    first = core_ref[0] == 0
    for p in range(groups):
        mine, theirs = mine_ref[p, :lines], theirs_ref[p, :lines]
        start = 2 * p * lines
        out_ref[start : start + lines, :] = jnp.where(first, mine, theirs)
        out_ref[start + lines : start + 2 * lines, :] = jnp.where(first, theirs, mine)
    lane = lax.broadcasted_iota(jnp.int32, (SUB, BLOCK), 1)
    line = lax.broadcasted_iota(jnp.int32, (SUB, BLOCK), 0)
    below = lax.broadcasted_iota(jnp.int32, (BLOCK, BLOCK), 0)
    right = lax.broadcasted_iota(jnp.int32, (BLOCK, BLOCK), 1)

    @pl.loop(0, blocks)
    def _(k):
        here = pl.ds(pl.multiple_of(k * BLOCK, BLOCK), BLOCK)
        tile_ref[...] = out_ref[here, here]
        for s in range(BLOCK // SUB):
            low, high = s * SUB, (s + 1) * SUB
            tile = tile_ref[low:high, :]
            unit = (lane - low == line).astype(jnp.float32)
            panel = jnp.where((lane >= low) & (lane < high), unit, tile)
            done = eliminated(tile, panel, low)
            tile_ref[low:high, :] = done
            if high < BLOCK:
                gone = right[high:, :] // SUB == s
                rest = jnp.where(gone, 0.0, tile_ref[high:, :])
                tile_ref[high:, :] = rest - dot(done.T[high:, :], done, ((1,), (0,)), EXACT)
        own = jnp.where(right <= below, tile_ref[...], 0.0)
        out_ref[here, :] = dot(own, out_ref[here, :], ((1,), (0,)), EXACT)
        out_ref[here, here] = own

        @pl.loop(k + 1, blocks)
        def _(i):
            there = pl.ds(pl.multiple_of(i * BLOCK, BLOCK), BLOCK)
            panel = out_ref[here, there].T
            out_ref[there, here] = jnp.zeros((BLOCK, BLOCK), jnp.float32)
            out_ref[there, :] = out_ref[there, :] - dot(panel, out_ref[here, :], ((1,), (0,)), EXACT)

    for k in range(blocks):
        here = slice(k * BLOCK, (k + 1) * BLOCK)
        whole = out_ref[here, :]
        lower = lax.broadcasted_iota(jnp.int32, whole.shape, 1) <= (
            lax.broadcasted_iota(jnp.int32, whole.shape, 0) + k * BLOCK
        )
        out_ref[here, :] = jnp.where(lower, whole, 0.0)


def inverse_factor(lines, core, mine, theirs):
    size = mine.shape[-1]
    return pl.pallas_call(
        functools.partial(factor_kernel, size // BLOCK, lines),
        out_shape=jax.ShapeDtypeStruct((size, size), jnp.float32),
        in_specs=[pl.BlockSpec(memory_space=pltpu.SMEM)]
        + [pl.BlockSpec(memory_space=pltpu.VMEM)] * 2,
        out_specs=pl.BlockSpec(memory_space=pltpu.VMEM),
        scratch_shapes=[pltpu.VMEM((BLOCK, BLOCK), jnp.float32)],
        cost_estimate=pl.CostEstimate(
            flops=1_000_000_000, bytes_accessed=8 * size * size, transcendentals=0
        ),
        name="inverse_factor",
    )(core, mine, theirs)


def summed_at_owner(x, axes):
    return jnp.sum(lax.all_to_all(x, axes, 0, 0, tiled=True), axis=0)


def from_all(x, axes):
    peers = lax.axis_size(axes)
    return lax.all_to_all(jnp.broadcast_to(x[None], (peers, *x.shape)), axes, 0, 0, tiled=True)


def from_other_core(x):
    return lax.ppermute(x, "row_1", [(0, 1), (1, 0)])


def shifted(x, axis, step):
    peers = lax.axis_size(axis)
    return lax.ppermute(x, axis, [(i, (i + step) % peers) for i in range(peers)])


def sum_over(x, axis):
    terms = [shifted(x, axis, step) for step in range(1, lax.axis_size(axis))]
    return sum(terms, x)


def around(index, axis):
    return index & (lax.axis_size(axis) - 1)


def replica_terms(x):
    peers, me = lax.axis_size("rep"), lax.axis_index("rep")
    width = x.shape[1] // peers
    cut = x.shape[0] // 2

    def part(step):
        return lax.dynamic_slice_in_dim(x, around(me + step, "rep") * width, width, 1)

    near = [shifted(part(step), "rep", step) for step in (1, -1)]
    far = part(2)
    above, below = shifted(far[:cut], "rep", 1), shifted(far[cut:], "rep", -1)
    far = [shifted(above, "rep", 1), shifted(below, "rep", -1)]
    return [part(0), *near, jnp.concatenate(far)]


def gathered_by_ring(block, core):
    peers, me = lax.axis_size("rep"), lax.axis_index("rep")
    lines, rank = block.shape
    cut = lines // 2
    whole = jnp.zeros((peers, 2, lines, rank), block.dtype)

    def both(whole, part, step, line):
        replica = around(me + step, "rep")
        for side, term in ((core, part), (1 - core, from_other_core(part))):
            whole = lax.dynamic_update_slice(whole, term[None, None], (replica, side, line, 0))
        return whole

    upper, lower = block[:cut], block[cut:]
    up_upper, down_lower = shifted(upper, "rep", 1), shifted(lower, "rep", -1)
    up_lower, down_upper = shifted(lower, "rep", 1), shifted(upper, "rep", -1)
    far_upper, far_lower = shifted(up_upper, "rep", 1), shifted(down_lower, "rep", -1)
    whole = both(whole, block, 0, 0)
    whole = both(whole, up_upper, -1, 0)
    whole = both(whole, down_lower, 1, cut)
    whole = both(whole, up_lower, -1, cut)
    whole = both(whole, down_upper, 1, 0)
    whole = both(whole, far_upper, -2, 0)
    return both(whole, far_lower, 2, cut)


def shards(acts, grad_out, momentum, q_basis):
    core = lax.axis_index("row_1")
    grad = dot(acts[0], grad_out[0], ((0,), (0,)))
    boosted = (momentum[0].astype(jnp.float32) + grad).astype(jnp.bfloat16)
    height, width = boosted.shape
    rank = q_basis.shape[0]
    replicas, columns = lax.axis_size("rep"), lax.axis_size("col")
    plane = replicas * columns
    strip = width // (2 * replicas)

    terms = replica_terms(boosted)

    partial_left = dot(boosted, q_basis, ((1,), (1,)))
    mine = summed_at_owner(partial_left.reshape(plane, height // plane, rank), PLANE)
    left = from_all(mine, PLANE).reshape(height, rank)

    lines = rank // (2 * plane)
    place = lax.axis_index("rep") * columns + lax.axis_index("col")
    own = lax.dynamic_slice_in_dim(left, place * 2 * lines, 2 * lines, 1)
    chunk = dot(own, left, ((0,), (0,)), EXACT)
    kept = lax.dynamic_slice_in_dim(chunk, core * lines, lines, 0)
    given = lax.dynamic_slice_in_dim(chunk, (1 - core) * lines, lines, 0)
    pair = kept + from_other_core(given)
    half = jnp.sum(from_all(pair, "row_0"), axis=0)
    known = from_all(jnp.pad(half, ((0, -lines % 8), (0, 0))), PLANE)
    inverse = inverse_factor(lines, core.reshape(1), known, from_other_core(known))

    total = sum(term.astype(jnp.float32) for term in terms)
    product = dot(total, left, ((0,), (0,)), CLOSE)
    first = core == 0
    ours = jnp.where(first, product[:strip], product[strip:])
    other = jnp.where(first, product[strip:], product[:strip])
    chips = lax.axis_size("row_0")
    parts = (ours + from_other_core(other)).reshape(chips, strip // chips, rank)
    arrived = lax.all_to_all(parts, "row_0", 0, 0, tiled=True)
    share = jnp.sum(arrived, axis=0)

    ortho = dot(left, inverse, ((1,), (1,)), CLOSE).astype(jnp.bfloat16)
    piece = (dot(share, inverse, ((1,), (1,)), CLOSE) * (1.0 / replicas)).astype(jnp.bfloat16)
    right = gathered_by_ring(from_all(piece, "row_0").reshape(strip, rank), core).reshape(width, rank)

    wide = right.astype(jnp.float32)
    squares = sum_over(jnp.sum(wide * wide, axis=0), "col")
    scale = lax.rsqrt(squares / (width * columns) + 1e-06)
    feedback = dot(ortho, right, ((1,), (1,)))
    momentum_next = (boosted.astype(jnp.float32) - (1.0 - keep_factor) * feedback).astype(
        jnp.bfloat16
    )[None]
    rows = rank // lax.axis_size(ROW)
    wanted = lax.axis_index(ROW) * rows + lax.broadcasted_iota(jnp.int32, (rows, rank), 0)
    chosen = lax.broadcasted_iota(jnp.int32, (rows, rank), 1) == wanted
    own_scale = jnp.sum(jnp.where(chosen, scale[None, :], 0.0), axis=1)
    q_own = dot(chosen.astype(jnp.bfloat16), right, ((1,), (1,)))
    q_next = (q_own * own_scale[:, None]).astype(jnp.bfloat16)
    height_all = height * lax.axis_size(ROW)
    scaled = (ortho.astype(jnp.float32) * scale[None, :]).astype(jnp.bfloat16)
    update = (
        jnp.sqrt(jnp.float32(height_all) / rank) * dot(scaled, right, ((1,), (1,)))
    ).astype(jnp.bfloat16)
    return (momentum_next, q_next, update)


def solution(mesh):
    split = Mesh(
        mesh.devices.reshape(mesh.shape["rep"], 8, 2, mesh.shape["col"]),
        ("rep", "row_0", "row_1", "col"),
    )

    return jax.shard_map(
        shards,
        mesh=split,
        in_specs=(P("rep", None, ROW), P("rep", None, "col"), P("rep", ROW, "col"), P(None, "col")),
        out_specs=(P("rep", ROW, "col"), P(ROW, "col"), P(ROW, "col")),
        check_vma=False,
    )
```

```python
import functools

import jax
import jax.numpy as jnp
from jax import lax
from jax.experimental import pallas as pl
from jax.experimental.pallas import tpu as pltpu
from jax.sharding import Mesh
from jax.sharding import PartitionSpec as P


ROW = ("row_0", "row_1")
PLANE = ("rep", "col")
BLOCK = 128
SUB = 32
WINDOW = 384
EXACT = lax.Precision.HIGHEST
CLOSE = lax.Precision.HIGH

keep_factor = 0.6


def dot(a, b, dims, precision=None):
    return lax.dot_general(
        a,
        b,
        (dims, ((), ())),
        precision=precision,
        preferred_element_type=jnp.float32,
    )


def eliminated(tile, panel, first):
    groups = SUB // 8
    row = lax.broadcasted_iota(jnp.int32, (8, BLOCK), 0)

    def spread(x, at):
        return jnp.broadcast_to(x[at : at + 1, :], (8, BLOCK))

    column = [[None] * groups for _ in range(SUB)]
    factor = [[None] * groups for _ in range(SUB)]
    kept = [panel[8 * g : 8 * g + 8, :] for g in range(groups)]
    pivots = [None] * groups
    for k in range(SUB):
        own, at = divmod(k, 8)
        for g in range(own, groups):
            lone = tile[8 * g : 8 * g + 8, first + k : first + k + 1]
            column[k][g] = jnp.broadcast_to(lone, (8, BLOCK))
        for j in range(k):
            across = spread(column[j][own], at)
            for g in range(own, groups):
                column[k][g] = column[k][g] - factor[j][g] * across
        pivot = spread(column[k][own], at)
        pivots[own] = pivot if at == 0 else jnp.where(row == at, pivot, pivots[own])
        inverse = 1.0 / pivot
        source = spread(kept[own], at)
        for g in range(own, groups):
            scaled = column[k][g] * inverse
            if g == own:
                scaled = jnp.where(row > at, scaled, 0.0)
            factor[k][g] = scaled
            kept[g] = kept[g] - scaled * source
    out = []
    for g in range(groups):
        y = lax.rsqrt(pivots[g])
        y = y * (1.5 - 0.5 * pivots[g] * y * y)
        out.append(kept[g] * y)
    return jnp.concatenate(out, axis=0)


def factor_kernel(blocks, lines, core_ref, mine_ref, theirs_ref, out_ref, tile_ref):
    first = core_ref[0] == 0
    size = out_ref.shape[1]

    @pl.loop(0, mine_ref.shape[0])
    def _(p):
        mine, theirs = mine_ref[p], theirs_ref[p]
        rest = jnp.zeros((mine.shape[0], size - mine.shape[1]), jnp.float32)
        pieces = []
        for half, piece in enumerate(
            (jnp.where(first, mine, theirs), jnp.where(first, theirs, mine))
        ):
            shift = (2 * p + half) * lines
            pieces.append(pltpu.roll(jnp.concatenate([piece, rest], 1), shift, 1)[:lines])
        start = pl.multiple_of(2 * p * lines, 8)
        out_ref[pl.ds(start, 2 * lines), :] = jnp.concatenate(pieces)

    @pl.loop(0, blocks)
    def _(i):
        here = pl.ds(pl.multiple_of(i * BLOCK, BLOCK), BLOCK)

        def mirrored(there):
            known = out_ref[here, there]
            out_ref[here, there] = jnp.where(known != 0.0, known, out_ref[there, here].T)

        mirrored(here)

        @pl.loop(i + 2, blocks)
        def _(j):
            mirrored(pl.ds(pl.multiple_of(j * BLOCK, BLOCK), BLOCK))

    lane = lax.broadcasted_iota(jnp.int32, (SUB, BLOCK), 1)
    line = lax.broadcasted_iota(jnp.int32, (SUB, BLOCK), 0)
    below = lax.broadcasted_iota(jnp.int32, (BLOCK, BLOCK), 0)
    right = lax.broadcasted_iota(jnp.int32, (BLOCK, BLOCK), 1)

    @pl.loop(0, blocks)
    def _(k):
        here = pl.ds(pl.multiple_of(k * BLOCK, BLOCK), BLOCK)
        tile_ref[...] = out_ref[here, here]
        for s in range(BLOCK // SUB):
            low, high = s * SUB, (s + 1) * SUB
            tile = tile_ref[low:high, :]
            unit = (lane - low == line).astype(jnp.float32)
            panel = jnp.where((lane >= low) & (lane < high), unit, tile)
            done = eliminated(tile, panel, low)
            tile_ref[low:high, :] = done
            if high < BLOCK:
                gone = right[high:, :] // SUB == s
                rest = jnp.where(gone, 0.0, tile_ref[high:, :])
                tile_ref[high:, :] = rest - dot(done.T[high:, :], done, ((1,), (0,)), EXACT)
        own = jnp.where(right <= below, tile_ref[...], 0.0)
        out_ref[here, :] = dot(own, out_ref[here, :], ((1,), (0,)), EXACT)
        out_ref[here, here] = own

        @pl.loop(k + 1, blocks)
        def _(i):
            there = pl.ds(pl.multiple_of(i * BLOCK, BLOCK), BLOCK)
            panel = out_ref[here, there].T
            out_ref[there, here] = jnp.zeros((BLOCK, BLOCK), jnp.float32)
            out_ref[there, :] = out_ref[there, :] - dot(panel, out_ref[here, :], ((1,), (0,)), EXACT)

    for k in range(blocks):
        here = slice(k * BLOCK, (k + 1) * BLOCK)
        whole = out_ref[here, :]
        lower = lax.broadcasted_iota(jnp.int32, whole.shape, 1) <= (
            lax.broadcasted_iota(jnp.int32, whole.shape, 0) + k * BLOCK
        )
        out_ref[here, :] = jnp.where(lower, whole, 0.0)


def inverse_factor(lines, size, core, mine, theirs):
    return pl.pallas_call(
        functools.partial(factor_kernel, size // BLOCK, lines),
        out_shape=jax.ShapeDtypeStruct((size, size), jnp.float32),
        in_specs=[pl.BlockSpec(memory_space=pltpu.SMEM)]
        + [pl.BlockSpec(memory_space=pltpu.VMEM)] * 2,
        out_specs=pl.BlockSpec(memory_space=pltpu.VMEM),
        scratch_shapes=[pltpu.VMEM((BLOCK, BLOCK), jnp.float32)],
        cost_estimate=pl.CostEstimate(
            flops=1_000_000_000, bytes_accessed=8 * size * size, transcendentals=0
        ),
        name="inverse_factor",
    )(core, mine, theirs)


def summed_at_owner(x, axes):
    return jnp.sum(lax.all_to_all(x, axes, 0, 0, tiled=True), axis=0)


def from_all(x, axes):
    peers = lax.axis_size(axes)
    return lax.all_to_all(jnp.broadcast_to(x[None], (peers, *x.shape)), axes, 0, 0, tiled=True)


def from_other_core(x):
    return lax.ppermute(x, "row_1", [(0, 1), (1, 0)])


def shifted(x, axis, step):
    peers = lax.axis_size(axis)
    return lax.ppermute(x, axis, [(i, (i + step) % peers) for i in range(peers)])


def sum_over(x, axis):
    terms = [shifted(x, axis, step) for step in range(1, lax.axis_size(axis))]
    return sum(terms, x)


def around(index, axis):
    return index & (lax.axis_size(axis) - 1)


def replica_terms(x):
    peers, me = lax.axis_size("rep"), lax.axis_index("rep")
    width = x.shape[1] // peers
    cut = x.shape[0] // 2

    def part(step):
        return lax.dynamic_slice_in_dim(x, around(me + step, "rep") * width, width, 1)

    near = [shifted(part(step), "rep", step) for step in (1, -1)]
    far = part(2)
    above, below = shifted(far[:cut], "rep", 1), shifted(far[cut:], "rep", -1)
    far = [shifted(above, "rep", 1), shifted(below, "rep", -1)]
    return [part(0), *near, jnp.concatenate(far)]


def gathered_by_ring(block, core):
    peers, me = lax.axis_size("rep"), lax.axis_index("rep")
    lines, rank = block.shape
    cut = lines // 2
    whole = jnp.zeros((peers, 2, lines, rank), block.dtype)

    def both(whole, part, step, line):
        replica = around(me + step, "rep")
        for side, term in ((core, part), (1 - core, from_other_core(part))):
            whole = lax.dynamic_update_slice(whole, term[None, None], (replica, side, line, 0))
        return whole

    upper, lower = block[:cut], block[cut:]
    up_upper, down_lower = shifted(upper, "rep", 1), shifted(lower, "rep", -1)
    up_lower, down_upper = shifted(lower, "rep", 1), shifted(upper, "rep", -1)
    far_upper, far_lower = shifted(up_upper, "rep", 1), shifted(down_lower, "rep", -1)
    whole = both(whole, block, 0, 0)
    whole = both(whole, up_upper, -1, 0)
    whole = both(whole, down_lower, 1, cut)
    whole = both(whole, up_lower, -1, cut)
    whole = both(whole, down_upper, 1, 0)
    whole = both(whole, far_upper, -2, 0)
    return both(whole, far_lower, 2, cut)


def shards(acts, grad_out, momentum, q_basis):
    core = lax.axis_index("row_1")
    grad = dot(acts[0], grad_out[0], ((0,), (0,)))
    boosted = (momentum[0].astype(jnp.float32) + grad).astype(jnp.bfloat16)
    height, width = boosted.shape
    rank = q_basis.shape[0]
    replicas, columns = lax.axis_size("rep"), lax.axis_size("col")
    plane = replicas * columns
    strip = width // (2 * replicas)

    terms = replica_terms(boosted)

    partial_left = dot(boosted, q_basis, ((1,), (1,)))
    mine = summed_at_owner(partial_left.reshape(plane, height // plane, rank), PLANE)
    left = from_all(mine, PLANE).reshape(height, rank)

    lines = rank // (2 * plane)
    place = lax.axis_index("rep") * columns + lax.axis_index("col")
    own = lax.dynamic_slice_in_dim(left, place * 2 * lines, 2 * lines, 1)
    chunk = dot(own, left, ((0,), (0,)), EXACT)
    around_chunk = jnp.concatenate([chunk, chunk], axis=1)

    def window(side):
        start = (side * lines, (2 * place + side) * lines)
        return lax.dynamic_slice(around_chunk, start, (lines, WINDOW))

    kept, given = window(core), window(1 - core)
    pair = kept + from_other_core(given)
    half = jnp.sum(from_all(pair, "row_0"), axis=0)
    known = from_all(jnp.pad(half, ((0, -lines % 8), (0, 0))), PLANE)
    inverse = inverse_factor(lines, rank, core.reshape(1), known, from_other_core(known))

    total = sum(term.astype(jnp.float32) for term in terms)
    product = dot(total, left, ((0,), (0,)), CLOSE)
    first = core == 0
    ours = jnp.where(first, product[:strip], product[strip:])
    other = jnp.where(first, product[strip:], product[:strip])
    chips = lax.axis_size("row_0")
    parts = (ours + from_other_core(other)).reshape(chips, strip // chips, rank)
    arrived = lax.all_to_all(parts, "row_0", 0, 0, tiled=True)
    share = jnp.sum(arrived, axis=0)

    ortho = dot(left, inverse, ((1,), (1,)), CLOSE).astype(jnp.bfloat16)
    piece = (dot(share, inverse, ((1,), (1,)), CLOSE) * (1.0 / replicas)).astype(jnp.bfloat16)
    right = gathered_by_ring(from_all(piece, "row_0").reshape(strip, rank), core).reshape(width, rank)

    wide = right.astype(jnp.float32)
    squares = sum_over(jnp.sum(wide * wide, axis=0), "col")
    scale = lax.rsqrt(squares / (width * columns) + 1e-06)
    feedback = dot(ortho, right, ((1,), (1,)))
    momentum_next = (boosted.astype(jnp.float32) - (1.0 - keep_factor) * feedback).astype(
        jnp.bfloat16
    )[None]
    rows = rank // lax.axis_size(ROW)
    wanted = lax.axis_index(ROW) * rows + lax.broadcasted_iota(jnp.int32, (rows, rank), 0)
    chosen = lax.broadcasted_iota(jnp.int32, (rows, rank), 1) == wanted
    own_scale = jnp.sum(jnp.where(chosen, scale[None, :], 0.0), axis=1)
    q_own = dot(chosen.astype(jnp.bfloat16), right, ((1,), (1,)))
    q_next = (q_own * own_scale[:, None]).astype(jnp.bfloat16)
    height_all = height * lax.axis_size(ROW)
    scaled = (ortho.astype(jnp.float32) * scale[None, :]).astype(jnp.bfloat16)
    update = (
        jnp.sqrt(jnp.float32(height_all) / rank) * dot(scaled, right, ((1,), (1,)))
    ).astype(jnp.bfloat16)
    return (momentum_next, q_next, update)


def solution(mesh):
    split = Mesh(
        mesh.devices.reshape(mesh.shape["rep"], 8, 2, mesh.shape["col"]),
        ("rep", "row_0", "row_1", "col"),
    )

    return jax.shard_map(
        shards,
        mesh=split,
        in_specs=(P("rep", None, ROW), P("rep", None, "col"), P("rep", ROW, "col"), P(None, "col")),
        out_specs=(P("rep", ROW, "col"), P(ROW, "col"), P(ROW, "col")),
        check_vma=False,
    )
```

```python
import functools
import math

import jax
import jax.numpy as jnp
from jax import lax
from jax.experimental import pallas as pl
from jax.experimental.pallas import tpu as pltpu
from jax.sharding import Mesh
from jax.sharding import PartitionSpec as P


ROW = ("row_0", "row_1")
PLANE = ("rep", "col")
BLOCK = 128
SUB = 32
WINDOW = 384
TILE = 384
EXACT = lax.Precision.HIGHEST
CLOSE = lax.Precision.HIGH

keep_factor = 0.6


def dot(a, b, dims, precision=None):
    return lax.dot_general(
        a,
        b,
        (dims, ((), ())),
        precision=precision,
        preferred_element_type=jnp.float32,
    )


def eliminated(tile, panel, first):
    groups = SUB // 8
    row = lax.broadcasted_iota(jnp.int32, (8, BLOCK), 0)

    def spread(x, at):
        return jnp.broadcast_to(x[at : at + 1, :], (8, BLOCK))

    column = [[None] * groups for _ in range(SUB)]
    factor = [[None] * groups for _ in range(SUB)]
    kept = [panel[8 * g : 8 * g + 8, :] for g in range(groups)]
    pivots = [None] * groups
    for k in range(SUB):
        own, at = divmod(k, 8)
        for g in range(own, groups):
            lone = tile[8 * g : 8 * g + 8, first + k : first + k + 1]
            column[k][g] = jnp.broadcast_to(lone, (8, BLOCK))
        for j in range(k):
            across = spread(column[j][own], at)
            for g in range(own, groups):
                column[k][g] = column[k][g] - factor[j][g] * across
        pivot = spread(column[k][own], at)
        pivots[own] = pivot if at == 0 else jnp.where(row == at, pivot, pivots[own])
        inverse = 1.0 / pivot
        source = spread(kept[own], at)
        for g in range(own, groups):
            scaled = column[k][g] * inverse
            if g == own:
                scaled = jnp.where(row > at, scaled, 0.0)
            factor[k][g] = scaled
            kept[g] = kept[g] - scaled * source
    out = []
    for g in range(groups):
        y = lax.rsqrt(pivots[g])
        y = y * (1.5 - 0.5 * pivots[g] * y * y)
        out.append(kept[g] * y)
    return jnp.concatenate(out, axis=0)


def factor_kernel(blocks, lines, core_ref, mine_ref, theirs_ref, out_ref, tile_ref):
    first = core_ref[0] == 0
    size = out_ref.shape[1]

    @pl.loop(0, mine_ref.shape[0])
    def _(p):
        mine, theirs = mine_ref[p], theirs_ref[p]
        rest = jnp.zeros((mine.shape[0], size - mine.shape[1]), jnp.float32)
        pieces = []
        for half, piece in enumerate(
            (jnp.where(first, mine, theirs), jnp.where(first, theirs, mine))
        ):
            shift = (2 * p + half) * lines
            pieces.append(pltpu.roll(jnp.concatenate([piece, rest], 1), shift, 1)[:lines])
        start = pl.multiple_of(2 * p * lines, 8)
        out_ref[pl.ds(start, 2 * lines), :] = jnp.concatenate(pieces)

    @pl.loop(0, blocks)
    def _(i):
        here = pl.ds(pl.multiple_of(i * BLOCK, BLOCK), BLOCK)

        def mirrored(there):
            known = out_ref[here, there]
            out_ref[here, there] = jnp.where(known != 0.0, known, out_ref[there, here].T)

        mirrored(here)

        @pl.loop(i + 2, blocks)
        def _(j):
            mirrored(pl.ds(pl.multiple_of(j * BLOCK, BLOCK), BLOCK))

    lane = lax.broadcasted_iota(jnp.int32, (SUB, BLOCK), 1)
    line = lax.broadcasted_iota(jnp.int32, (SUB, BLOCK), 0)
    below = lax.broadcasted_iota(jnp.int32, (BLOCK, BLOCK), 0)
    right = lax.broadcasted_iota(jnp.int32, (BLOCK, BLOCK), 1)

    @pl.loop(0, blocks)
    def _(k):
        here = pl.ds(pl.multiple_of(k * BLOCK, BLOCK), BLOCK)
        tile_ref[...] = out_ref[here, here]
        for s in range(BLOCK // SUB):
            low, high = s * SUB, (s + 1) * SUB
            tile = tile_ref[low:high, :]
            unit = (lane - low == line).astype(jnp.float32)
            panel = jnp.where((lane >= low) & (lane < high), unit, tile)
            done = eliminated(tile, panel, low)
            tile_ref[low:high, :] = done
            if high < BLOCK:
                gone = right[high:, :] // SUB == s
                rest = jnp.where(gone, 0.0, tile_ref[high:, :])
                tile_ref[high:, :] = rest - dot(done.T[high:, :], done, ((1,), (0,)), EXACT)
        own = jnp.where(right <= below, tile_ref[...], 0.0)
        out_ref[here, :] = dot(own, out_ref[here, :], ((1,), (0,)), EXACT)
        out_ref[here, here] = own

        @pl.loop(k + 1, blocks)
        def _(i):
            there = pl.ds(pl.multiple_of(i * BLOCK, BLOCK), BLOCK)
            panel = out_ref[here, there].T
            out_ref[there, here] = jnp.zeros((BLOCK, BLOCK), jnp.float32)
            out_ref[there, :] = out_ref[there, :] - dot(panel, out_ref[here, :], ((1,), (0,)), EXACT)

    for k in range(blocks):
        here = slice(k * BLOCK, (k + 1) * BLOCK)
        whole = out_ref[here, :]
        lower = lax.broadcasted_iota(jnp.int32, whole.shape, 1) <= (
            lax.broadcasted_iota(jnp.int32, whole.shape, 0) + k * BLOCK
        )
        out_ref[here, :] = jnp.where(lower, whole, 0.0)


def inverse_factor(lines, size, core, mine, theirs):
    return pl.pallas_call(
        functools.partial(factor_kernel, size // BLOCK, lines),
        out_shape=jax.ShapeDtypeStruct((size, size), jnp.float32),
        in_specs=[pl.BlockSpec(memory_space=pltpu.SMEM)]
        + [pl.BlockSpec(memory_space=pltpu.VMEM)] * 2,
        out_specs=pl.BlockSpec(memory_space=pltpu.VMEM),
        scratch_shapes=[pltpu.VMEM((BLOCK, BLOCK), jnp.float32)],
        cost_estimate=pl.CostEstimate(
            flops=1_000_000_000, bytes_accessed=8 * size * size, transcendentals=0
        ),
        name="inverse_factor",
    )(core, mine, theirs)


def outputs_kernel(
    grow, ortho_ref, scaled_ref, chosen_ref, scale_ref, right_ref, boosted_ref, next_ref, q_ref, step_ref
):
    across = ((1,), (1,))
    right = right_ref[...]
    feedback = dot(ortho_ref[...], right, across)
    kept = boosted_ref[...].astype(jnp.float32) - (1.0 - keep_factor) * feedback
    next_ref[...] = kept.astype(jnp.bfloat16)
    q_ref[...] = (dot(chosen_ref[...], right, across) * scale_ref[...]).astype(jnp.bfloat16)
    step_ref[...] = (grow * dot(scaled_ref[...], right, across)).astype(jnp.bfloat16)


def outputs(grow, ortho, scaled, chosen, own_scale, right, boosted):
    width, rank = right.shape
    height, rows = ortho.shape[0], chosen.shape[0]

    def whole(x):
        return pl.BlockSpec(x.shape, lambda i: (0, 0))

    def strip(lines):
        return pl.BlockSpec((lines, TILE), lambda i: (0, i))

    return pl.pallas_call(
        functools.partial(outputs_kernel, grow),
        grid=(width // TILE,),
        in_specs=[whole(x) for x in (ortho, scaled, chosen, own_scale)]
        + [pl.BlockSpec((TILE, rank), lambda i: (i, 0)), strip(height)],
        out_specs=[strip(height), strip(rows), strip(height)],
        out_shape=[
            jax.ShapeDtypeStruct((lines, width), jnp.bfloat16) for lines in (height, rows, height)
        ],
        cost_estimate=pl.CostEstimate(
            flops=2 * (2 * height + rows) * rank * width,
            bytes_accessed=2 * width * (rank + 3 * height + rows),
            transcendentals=0,
        ),
        name="outputs",
    )(ortho, scaled, chosen, own_scale, right, boosted)


def summed_at_owner(x, axes):
    return jnp.sum(lax.all_to_all(x, axes, 0, 0, tiled=True), axis=0)


def from_all(x, axes):
    peers = lax.axis_size(axes)
    return lax.all_to_all(jnp.broadcast_to(x[None], (peers, *x.shape)), axes, 0, 0, tiled=True)


def from_other_core(x):
    return lax.ppermute(x, "row_1", [(0, 1), (1, 0)])


def shifted(x, axis, step):
    peers = lax.axis_size(axis)
    return lax.ppermute(x, axis, [(i, (i + step) % peers) for i in range(peers)])


def sum_over(x, axis):
    terms = [shifted(x, axis, step) for step in range(1, lax.axis_size(axis))]
    return sum(terms, x)


def around(index, axis):
    return index & (lax.axis_size(axis) - 1)


def doubled(x, low_at):
    high = x.astype(jnp.bfloat16)
    low = (x - lax.reduce_precision(x, 8, 7)).astype(jnp.bfloat16)
    return jnp.concatenate([high, low, high] if low_at else [high, high, low])


def replica_terms(x):
    peers, me = lax.axis_size("rep"), lax.axis_index("rep")
    width = x.shape[1] // peers
    cut = x.shape[0] // 2

    def part(step):
        return lax.dynamic_slice_in_dim(x, around(me + step, "rep") * width, width, 1)

    near = [shifted(part(step), "rep", step) for step in (1, -1)]
    far = part(2)
    above, below = shifted(far[:cut], "rep", 1), shifted(far[cut:], "rep", -1)
    far = [shifted(above, "rep", 1), shifted(below, "rep", -1)]
    return [part(0), *near, jnp.concatenate(far)]


def gathered_by_ring(block, core):
    peers, me = lax.axis_size("rep"), lax.axis_index("rep")
    lines, rank = block.shape
    cut = lines // 2
    whole = jnp.zeros((peers, 2, lines, rank), block.dtype)

    def both(whole, part, step, line):
        replica = around(me + step, "rep")
        for side, term in ((core, part), (1 - core, from_other_core(part))):
            whole = lax.dynamic_update_slice(whole, term[None, None], (replica, side, line, 0))
        return whole

    upper, lower = block[:cut], block[cut:]
    up_upper, down_lower = shifted(upper, "rep", 1), shifted(lower, "rep", -1)
    up_lower, down_upper = shifted(lower, "rep", 1), shifted(upper, "rep", -1)
    far_upper, far_lower = shifted(up_upper, "rep", 1), shifted(down_lower, "rep", -1)
    whole = both(whole, block, 0, 0)
    whole = both(whole, up_upper, -1, 0)
    whole = both(whole, down_lower, 1, cut)
    whole = both(whole, up_lower, -1, cut)
    whole = both(whole, down_upper, 1, 0)
    whole = both(whole, far_upper, -2, 0)
    return both(whole, far_lower, 2, cut)


def shards(acts, grad_out, momentum, q_basis):
    core = lax.axis_index("row_1")
    grad = dot(acts[0], grad_out[0], ((0,), (0,)))
    boosted = (momentum[0].astype(jnp.float32) + grad).astype(jnp.bfloat16)
    height, width = boosted.shape
    rank = q_basis.shape[0]
    replicas, columns = lax.axis_size("rep"), lax.axis_size("col")
    plane = replicas * columns
    strip = width // (2 * replicas)

    terms = replica_terms(boosted)

    partial_left = dot(boosted, q_basis, ((1,), (1,)))
    mine = summed_at_owner(partial_left.reshape(plane, height // plane, rank), PLANE)
    left = from_all(mine, PLANE).reshape(height, rank)

    lines = rank // (2 * plane)
    place = lax.axis_index("rep") * columns + lax.axis_index("col")
    own = lax.dynamic_slice_in_dim(left, place * 2 * lines, 2 * lines, 1)
    chunk = dot(own, left, ((0,), (0,)), EXACT)
    around_chunk = jnp.concatenate([chunk, chunk], axis=1)

    def window(side):
        start = (side * lines, (2 * place + side) * lines)
        return lax.dynamic_slice(around_chunk, start, (lines, WINDOW))

    kept, given = window(core), window(1 - core)
    pair = kept + from_other_core(given)
    half = jnp.sum(from_all(pair, "row_0"), axis=0)
    known = from_all(jnp.pad(half, ((0, -lines % 8), (0, 0))), PLANE)
    inverse = inverse_factor(lines, rank, core.reshape(1), known, from_other_core(known))

    total = sum(term.astype(jnp.float32) for term in terms)
    product = dot(doubled(total, 1), doubled(left, 0), ((0,), (0,)))
    first = core == 0
    ours = jnp.where(first, product[:strip], product[strip:])
    other = jnp.where(first, product[strip:], product[:strip])
    chips = lax.axis_size("row_0")
    parts = (ours + from_other_core(other)).reshape(chips, strip // chips, rank)
    arrived = lax.all_to_all(parts, "row_0", 0, 0, tiled=True)
    share = jnp.sum(arrived, axis=0)

    ortho = dot(left, inverse, ((1,), (1,)), CLOSE).astype(jnp.bfloat16)
    ortho = lax.optimization_barrier(ortho)
    piece = (dot(share, inverse, ((1,), (1,)), CLOSE) * (1.0 / replicas)).astype(jnp.bfloat16)
    pieces = from_all(piece, "row_0")
    right = gathered_by_ring(pieces.reshape(strip, rank), core).reshape(width, rank)

    wide = right.astype(jnp.float32)
    squares = sum_over(jnp.sum(wide * wide, axis=0), "col")
    scale = lax.rsqrt(squares / (width * columns) + 1e-06)
    rows = rank // lax.axis_size(ROW)
    wanted = lax.axis_index(ROW) * rows + lax.broadcasted_iota(jnp.int32, (rows, rank), 0)
    chosen = lax.broadcasted_iota(jnp.int32, (rows, rank), 1) == wanted
    own_scale = jnp.sum(jnp.where(chosen, scale[None, :], 0.0), axis=1, keepdims=True)
    scaled = (ortho.astype(jnp.float32) * scale[None, :]).astype(jnp.bfloat16)
    grow = math.sqrt(height * lax.axis_size(ROW) / rank)
    momentum_next, q_next, update = outputs(
        grow, ortho, scaled, chosen.astype(jnp.bfloat16), own_scale, right, boosted
    )
    return (momentum_next[None], q_next, update)


def solution(mesh):
    split = Mesh(
        mesh.devices.reshape(mesh.shape["rep"], 8, 2, mesh.shape["col"]),
        ("rep", "row_0", "row_1", "col"),
    )

    return jax.shard_map(
        shards,
        mesh=split,
        in_specs=(P("rep", None, ROW), P("rep", None, "col"), P("rep", ROW, "col"), P(None, "col")),
        out_specs=(P("rep", ROW, "col"), P(ROW, "col"), P(ROW, "col")),
        check_vma=False,
    )
```
